32 devices in a mesh: batch: 8 (over z, x), mp: 4 (over y, core).
Axes of the slice: x: 2, y: 2, z: 4, core: 2. Of those that a mesh axis runs over, the one named last changes fastest.
Arguments:
- features: bfloat16 [1024, 65536], P('batch', 'mp'), may hold values from 0 to 4
- tiles: bfloat16 [2, 512, 3, 128, 128], P(None, 'mp', None, 'batch'), may hold values from -0.3125 to 0.3125
- biases: float32 [2, 65536], P(None, 'mp'), may hold values from -0.5 to 0
- in_block: int32 [2, 512, 3], replicated, may hold values from 0 to 511, as said below
Outputs:
- activations: bfloat16 [1024, 65536], P('batch', 'mp')
- row_means: float32 [1024], P('batch')
- grand: float32 [], replicated
The draws below stay inside these ranges and needn't reach their ends.
Inputs may be any that keep to these rules, and one draw needn't show every extreme that they name: `in_block`: number the 384 tiles of mp shard m (column blocks m * 128 to (m + 1) * 128 - 1) in order of column block, then tile slot; tile number s reads a block of shard s // 96, that is an id in [(s // 96) * 128, (s // 96 + 1) * 128).
All inputs are finite; a program needn't handle non-finite values.
Results may differ from the reference program's by a relative error of at most 0.0052.
Values may be sent and summed in bfloat16 or wider, within the bound.
A program may use at most 128 MiB of HBM per device.

```python
import math
import jax
import jax.numpy as jnp
from jax import lax

NEUR = 65536
BLOCK = 128
FAN_TILES = 3
LAYERS = 2
ROWS_DEV = 128
NB = 512
CB_DEV = 128
PER_PEER = 96
ROWS = 1024


def draw_in_block(key, part):
    shard_count = NB // CB_DEV
    slots = CB_DEV * FAN_TILES
    local = jax.random.randint(key, (LAYERS, shard_count, slots), 0, CB_DEV, dtype=jnp.int32)
    source = jnp.arange(slots, dtype=jnp.int32) // PER_PEER * CB_DEV
    ids = local + source[None, None, :]
    return ids.reshape(LAYERS, NB, FAN_TILES).astype(jnp.int32)


def draw_features(key, part):
    key_scale, key_base = jax.random.split(jax.random.fold_in(key, 17))
    groups = ROWS // ROWS_DEV
    logs = jax.random.uniform(key_scale, (groups, 1, 1), jnp.float32, math.log(0.25), math.log(2.0))
    scale = jnp.exp(logs)
    base = jax.random.uniform(key_base, (groups, ROWS_DEV, NEUR), jnp.float32, 0.0, 1.0)
    base = 2.0 * base
    values = jnp.clip(scale * base, 0.0, 4.0)
    return values.reshape(ROWS, NEUR).astype(jnp.bfloat16)


def levels(rng, extent, pieces, smallest, largest):
    def one(dim, blocks):
        steps = jax.random.uniform(jax.random.fold_in(jax.random.fold_in(rng, 6), dim), (blocks,), jnp.float32, smallest / len(pieces), largest / len(pieces))
        return jnp.repeat(jnp.exp(steps), extent[dim] // blocks).reshape((-1,) + (1,) * (len(extent) - dim - 1))

    level = one(*pieces[0])
    for cut in pieces[1:]:
        level = level * one(*cut)
    return level


def gaussian(stream_key, dims, spread, most, shards=(), kind=jnp.bfloat16):
    array = jax.random.normal(stream_key, dims, jnp.float32) * spread
    if len(shards) > 0:
        array = levels(stream_key, dims, shards, -0.22, 0.18) * array
    return jnp.clip(array, min=-most, max=most).astype(kind)


def setup_inputs(seed: int = 0) -> dict:
    seeds = jax.random.split(jax.random.key(seed), 5)
    return {
        "features": draw_features(jax.random.fold_in(seeds[4], 71), 0),
        "tiles": gaussian(seeds[1], (LAYERS, NB, FAN_TILES, BLOCK, BLOCK), (FAN_TILES * BLOCK) ** -0.5, 0.3125, ((1, 4), (3, 8))),
        "biases": jnp.clip(-0.5 + 0.5 * jax.random.uniform(seeds[2], (LAYERS, NEUR), jnp.float32) ** levels(seeds[2], (LAYERS, NEUR), ((1, 4),), -0.2, 0.2), -0.5, 0.0),
        "in_block": draw_in_block(jax.random.fold_in(seeds[4], 71), 0),
    }


def one_layer(current, tile_layer, bias_layer, ids_layer):
    group = math.gcd(NB, 32)
    blocks_all = current.reshape(ROWS, NB, BLOCK)
    ids_grouped = ids_layer.reshape(NB // group, group, FAN_TILES)
    tiles_grouped = tile_layer.reshape(NB // group, group, FAN_TILES, BLOCK, BLOCK)
    bias_grouped = bias_layer.reshape(NB // group, group, BLOCK)

    def per_group(packed):
        ids_here, tiles_here, bias_here = packed
        taken = jnp.take(blocks_all, ids_here.reshape(-1), axis=1)
        taken = taken.reshape(ROWS, group, FAN_TILES, BLOCK).astype(jnp.float32)
        total = jnp.einsum("rjki,jkio->rjo", taken, tiles_here.astype(jnp.float32))
        shifted = total + bias_here[None, :, :]
        return jnp.clip(shifted, 0.0, 32.0).astype(jnp.bfloat16)

    result = lax.map(per_group, (ids_grouped, tiles_grouped, bias_grouped))
    return jnp.transpose(result, (1, 0, 2, 3)).reshape(ROWS, NEUR)


def reference(features, tiles, biases, in_block):
    current = features
    for layer_no in range(LAYERS):
        current = one_layer(current, tiles[layer_no], biases[layer_no], in_block[layer_no])
    row_means = jnp.sum(current.astype(jnp.float32), axis=1) / NEUR
    grand = jnp.sum(row_means) / ROWS
    return current, row_means, grand
```

```python
import functools

import jax
import jax.numpy as jnp
from jax import lax
from jax.experimental import pallas as pl
from jax.experimental.pallas import tpu as pltpu
from jax.sharding import PartitionSpec as P

MESH = pl.DeviceIdType.MESH


def geometry(mesh):
    groups, shards = mesh.devices.shape
    where = [getattr(d, "coords", None) for d in mesh.devices[:, 0]]
    if groups == 1 or where[0] is None or where[0] == where[1]:
        return groups, 1, True, 1
    moved = [i for i in range(len(where[0])) if where[0][i] != where[1][i]][0]
    minor = 1
    while minor < groups and all(
        where[minor][i] == where[0][i] for i in range(len(where[0])) if i != moved
    ):
        minor += 1
    major = groups // minor
    row = [d.coords for d in mesh.devices[0, :]]
    cores = sum(1 for c in row if c == row[0])
    if major >= minor:
        return major, minor, True, cores
    return minor, major, False, cores


def gather_kernel(
    geo, shards, layer, pieces,
    tiles, cur, wout, xout,
    wv, xv, lsem, wrecv, wup, wdn, wcross, whalf, xrecv, xfar, xcore,
):
    nl, nq, line_major, nc = geo
    ny = shards // nc
    bi = lax.axis_index("batch")
    mi = lax.axis_index("mp")
    if line_major:
        l, q = bi // nq, bi % nq
    else:
        l, q = bi % nl, bi // nl
    y, core = mi // nc, mi % nc
    step_w = tiles.shape[1] // pieces
    step_x = cur.shape[0] // pieces
    halves = nq == 2 and nl % 2 == 0
    first = pieces // 2

    def group(level, side):
        return level * nq + side if line_major else side * nl + level

    sides = [(q + d) % nq for d in range(1, nq)]
    fars = [((y + d) % ny) * nc + core for d in range(1, ny)]
    partners = [y * nc + (core + d) % nc for d in range(1, nc)]

    barrier = pltpu.get_barrier_semaphore()

    def greet(b, m):
        pl.semaphore_signal(barrier, inc=1, device_id=(b, m), device_id_type=MESH)

    @pl.when(l > 0)
    def _():
        greet(group(l - 1, q), mi)

    @pl.when(l < nl - 1)
    def _():
        greet(group(l + 1, q), mi)

    for side in sides:
        greet(group(l, side), mi)
    for m in fars + partners:
        greet(bi, m)
    near = jnp.where(l > 0, 1, 0) + jnp.where(l < nl - 1, 1, 0)
    pl.semaphore_wait(barrier, len(sides) + len(fars) + len(partners) + near)

    in_w = pltpu.make_async_copy(tiles.at[layer], wv, lsem.at[0])
    in_x = pltpu.make_async_copy(cur, xv, lsem.at[1])
    in_w.start()
    in_x.start()

    def wcopy(own, b, c, to, ssem):
        part = pl.ds(c * step_w, step_w)
        return pltpu.make_async_remote_copy(
            src_ref=tiles.at[layer, part] if own else wout.at[b, part],
            dst_ref=wout.at[b, part],
            send_sem=ssem,
            recv_sem=wrecv.at[b, c],
            device_id=(to, mi),
            device_id_type=MESH,
        )

    def xcopy(own, m, c, to, ssem):
        part = pl.ds(c * step_x, step_x)
        return pltpu.make_async_remote_copy(
            src_ref=cur.at[part] if own else xout.at[m, part],
            dst_ref=xout.at[m, part],
            send_sem=ssem,
            recv_sem=xrecv.at[m, c],
            device_id=(bi, to),
            device_id_type=MESH,
        )

    def phase(p, c, drain):
        def go(copy):
            copy.wait_send() if drain else copy.start()

        def arrived_w(b):
            if not drain:
                wcopy(False, b, c, bi, wup.at[0, c]).wait_recv()

        if p == 0:
            @pl.when(l < nl - 1)
            def _():
                go(wcopy(True, bi, c, group(l + 1, q), wup.at[0, c]))

            @pl.when(l > 0)
            def _():
                go(wcopy(True, bi, c, group(l - 1, q), wdn.at[0, c]))

            for i, side in enumerate(sides):
                go(wcopy(True, bi, c, group(l, side), wcross.at[i, l, c]))
            for i, m in enumerate(fars):
                go(xcopy(True, mi, c, m, xfar.at[i, c]))
            for i, m in enumerate(partners):
                go(xcopy(True, mi, c, m, xcore.at[i, y, c]))
        else:
            @pl.when(l - p >= 0)
            def _():
                b = group(l - p, q)
                arrived_w(b)

                @pl.when(l < nl - 1)
                def _():
                    go(wcopy(False, b, c, group(l + 1, q), wup.at[p, c]))

                def across():
                    for i, side in enumerate(sides):
                        go(wcopy(False, b, c, group(l, side), wcross.at[i, l - p, c]))

                if halves and p == 1:
                    pl.when((l < nl // 2) | (c < first))(across)
                else:
                    across()

            @pl.when(l + p <= nl - 1)
            def _():
                b = group(l + p, q)
                arrived_w(b)

                @pl.when(l > 0)
                def _():
                    go(wcopy(False, b, c, group(l - 1, q), wdn.at[p, c]))

                def across():
                    for i, side in enumerate(sides):
                        go(wcopy(False, b, c, group(l, side), wcross.at[i, l + p, c]))

                if halves and p == 1:
                    pl.when((l >= nl // 2) | (c < first))(across)
                else:
                    across()

            if halves and p == 1:
                @pl.when(c >= first)
                def _():
                    b = group(l, sides[0])
                    arrived_w(b)

                    @pl.when((l + 1 >= nl // 2) & (l < nl - 1))
                    def _():
                        go(wcopy(False, b, c, group(l + 1, q), whalf.at[0, c]))

                    @pl.when((l - 1 < nl // 2) & (l > 0))
                    def _():
                        go(wcopy(False, b, c, group(l - 1, q), whalf.at[1, c]))

        if p == nl - 1:
            for d, far in enumerate(fars):
                if not drain:
                    xcopy(False, far, c, mi, xfar.at[0, c]).wait_recv()
                for i, m in enumerate(partners):
                    go(xcopy(False, far, c, m, xcore.at[i, far // nc, c]))

    for p in range(nl):
        @pl.loop(0, pieces)
        def _(c, p=p):
            phase(p, c, False)

        if p == 0:
            in_w.wait()
            in_x.wait()
            out_w = pltpu.make_async_copy(wv, wout.at[bi], lsem.at[2])
            out_x = pltpu.make_async_copy(xv, xout.at[mi], lsem.at[3])
            out_w.start()
            out_x.start()

    @pl.loop(0, pieces)
    def _(c):
        for side in sides:
            for level in range(nl):
                b = group(level, side)

                def arrive(b=b):
                    wcopy(False, b, c, bi, wup.at[0, c]).wait_recv()

                if halves:
                    pl.when((l != level) | (c < first))(arrive)
                else:
                    arrive()
        for m in partners:
            for yy in range(ny):
                xcopy(False, yy * nc + m % nc, c, mi, xfar.at[0, c]).wait_recv()

    out_w.wait()
    out_x.wait()
    for p in range(nl):
        @pl.loop(0, pieces)
        def _(c, p=p):
            phase(p, c, True)


def gather(geo, shards, groups, layer, tiles, cur):
    nl, nq, _, nc = geo
    pieces = 8 if groups <= 8 else 2
    ny = shards // nc
    dma = pltpu.SemaphoreType.DMA
    return pl.pallas_call(
        functools.partial(gather_kernel, geo, shards, layer, pieces),
        out_shape=(
            jax.ShapeDtypeStruct((groups,) + tiles.shape[1:], tiles.dtype),
            jax.ShapeDtypeStruct((shards,) + cur.shape, cur.dtype),
        ),
        in_specs=[pl.BlockSpec(memory_space=pl.ANY)] * 2,
        out_specs=(pl.BlockSpec(memory_space=pl.ANY),) * 2,
        scratch_shapes=[
            pltpu.VMEM(tiles.shape[1:], tiles.dtype),
            pltpu.VMEM(cur.shape, cur.dtype),
            dma((4,)),
            dma((groups, pieces)),
            dma((nl, pieces)),
            dma((nl, pieces)),
            dma((max(nq - 1, 1), nl, pieces)),
            dma((2, pieces)),
            dma((shards, pieces)),
            dma((max(ny - 1, 1), pieces)),
            dma((max(nc - 1, 1), ny, pieces)),
        ],
        compiler_params=pltpu.CompilerParams(collective_id=layer, has_side_effects=True),
        name=f"gather_{layer}",
    )(tiles, cur)


def layer_kernel(fan, batch_blocks, steps, ids, x_ref, w_ref, b_ref, o_ref, s_ref):
    step = pl.program_id(0) * steps + pl.program_id(1)
    side = w_ref.shape[4]

    @pl.when(step == 0)
    def _():
        s_ref[...] = jnp.zeros_like(s_ref)

    for j in range(batch_blocks):
        xs, ws = [], []
        for t in range(fan):
            at = ids[(step * batch_blocks + j) * fan + t]
            xs.append(x_ref[0, :, pl.ds(pl.multiple_of(at * side, side), side)])
            ws.append(w_ref[:, j, t].reshape(side, side))
        total = jnp.dot(
            jnp.concatenate(xs, axis=1),
            jnp.concatenate(ws, axis=0),
            preferred_element_type=jnp.float32,
        )
        cols = slice(j * side, (j + 1) * side)
        out = jnp.clip(total + b_ref[:, cols], 0.0, 32.0).astype(o_ref.dtype)
        o_ref[:, cols] = out
        s_ref[...] += out.astype(jnp.float32)


def apply_layer(ids, xall, wall, bias, blocks):
    shards, rows, width = xall.shape
    groups, cb, fan, share, side = wall.shape
    per_shard = cb // shards
    batch_blocks = min(blocks, per_shard)
    steps = per_shard // batch_blocks
    return pl.pallas_call(
        functools.partial(layer_kernel, fan, batch_blocks, steps),
        out_shape=(
            jax.ShapeDtypeStruct((rows, width), xall.dtype),
            jax.ShapeDtypeStruct((rows, side), jnp.float32),
        ),
        grid_spec=pltpu.PrefetchScalarGridSpec(
            num_scalar_prefetch=1,
            grid=(shards, steps),
            in_specs=[
                pl.BlockSpec((1, rows, width), lambda s, k, ids: (s, 0, 0)),
                pl.BlockSpec(
                    (groups, batch_blocks, fan, share, side),
                    lambda s, k, ids: (0, s * steps + k, 0, 0, 0),
                ),
                pl.BlockSpec((1, batch_blocks * side), lambda s, k, ids: (0, s * steps + k)),
            ],
            out_specs=(
                pl.BlockSpec((rows, batch_blocks * side), lambda s, k, ids: (0, s * steps + k)),
                pl.BlockSpec((rows, side), lambda s, k, ids: (0, 0)),
            ),
        ),
        compiler_params=pltpu.CompilerParams(
            dimension_semantics=("arbitrary", "arbitrary"), vmem_limit_bytes=48 * 1024 * 1024
        ),
    )(ids, xall, wall, bias)


def on_device(geo, features, tiles, biases, in_block):
    shards = lax.axis_size("mp")
    groups = lax.axis_size("batch")
    me = lax.axis_index("mp")
    rows = features.shape[0]
    side = tiles.shape[4]
    cb = tiles.shape[1]
    fan = tiles.shape[2]
    current = features
    mine = lax.dynamic_slice_in_dim(in_block, me * cb, cb, axis=1) % cb
    for layer in range(tiles.shape[0]):
        wall, xall = gather(geo, shards, groups, layer, tiles, current)
        current, sums = apply_layer(
            mine[layer].reshape(-1), xall, wall, biases[layer].reshape(1, -1), 8
        )
    spot = (jnp.arange(groups) == lax.axis_index("batch")).astype(jnp.float32)
    everyone = lax.psum(spot[:, None] * jnp.sum(sums, axis=1)[None, :], ("batch", "mp"))
    neurons = cb * side * shards
    row_means = (
        lax.dynamic_index_in_dim(everyone, lax.axis_index("batch"), 0, False) / neurons
    )
    grand = jnp.sum(everyone / neurons) / (rows * groups)
    return (current, row_means, grand)


def solution(mesh):
    placed = (P("batch", "mp"), P(None, "mp", None, "batch", None), P(None, "mp"), P())
    return jax.shard_map(
        functools.partial(on_device, geometry(mesh)),
        mesh=mesh,
        in_specs=placed,
        out_specs=(P("batch", "mp"), P("batch"), P()),
        check_vma=False,
    )
```

```python
import functools

import jax
import jax.numpy as jnp
from jax import lax
from jax.experimental import pallas as pl
from jax.experimental.pallas import tpu as pltpu
from jax.sharding import PartitionSpec as P

MESH = pl.DeviceIdType.MESH


def geometry(mesh):
    groups, shards = mesh.devices.shape
    where = [getattr(d, "coords", None) for d in mesh.devices[:, 0]]
    if groups == 1 or where[0] is None or where[0] == where[1]:
        return groups, 1, True, 1
    moved = [i for i in range(len(where[0])) if where[0][i] != where[1][i]][0]
    minor = 1
    while minor < groups and all(
        where[minor][i] == where[0][i] for i in range(len(where[0])) if i != moved
    ):
        minor += 1
    major = groups // minor
    row = [d.coords for d in mesh.devices[0, :]]
    cores = sum(1 for c in row if c == row[0])
    if major >= minor:
        return major, minor, True, cores
    return minor, major, False, cores


def gather_kernel(
    geo, shards, layer, pieces,
    tiles, cur, wout, xout,
    wv, xv, lsem, wrecv, wup, wdn, wcross, whalf, xrecv, xfar, xcore,
):
    nl, nq, line_major, nc = geo
    ny = shards // nc
    bi = lax.axis_index("batch")
    mi = lax.axis_index("mp")
    if line_major:
        l, q = bi // nq, bi % nq
    else:
        l, q = bi % nl, bi // nl
    y, core = mi // nc, mi % nc
    step_w = tiles.shape[1] // pieces
    step_x = cur.shape[0] // pieces
    halves = nq == 2 and nl % 2 == 0
    first = pieces // 2

    def group(level, side):
        return level * nq + side if line_major else side * nl + level

    sides = [(q + d) % nq for d in range(1, nq)]
    fars = [((y + d) % ny) * nc + core for d in range(1, ny)]
    partners = [y * nc + (core + d) % nc for d in range(1, nc)]

    barrier = pltpu.get_barrier_semaphore()

    def greet(b, m):
        pl.semaphore_signal(barrier, inc=1, device_id=(b, m), device_id_type=MESH)

    @pl.when(l > 0)
    def _():
        greet(group(l - 1, q), mi)

    @pl.when(l < nl - 1)
    def _():
        greet(group(l + 1, q), mi)

    for side in sides:
        greet(group(l, side), mi)
    for m in fars + partners:
        greet(bi, m)
    near = jnp.where(l > 0, 1, 0) + jnp.where(l < nl - 1, 1, 0)
    pl.semaphore_wait(barrier, len(sides) + len(fars) + len(partners) + near)

    in_w = pltpu.make_async_copy(tiles.at[layer], wv, lsem.at[0])
    in_x = pltpu.make_async_copy(cur, xv, lsem.at[1])
    in_w.start()
    in_x.start()

    def wcopy(own, b, c, to, ssem):
        part = pl.ds(c * step_w, step_w)
        return pltpu.make_async_remote_copy(
            src_ref=tiles.at[layer, part] if own else wout.at[b, part],
            dst_ref=wout.at[b, part],
            send_sem=ssem,
            recv_sem=wrecv.at[b, c],
            device_id=(to, mi),
            device_id_type=MESH,
        )

    def xcopy(own, m, c, to, ssem):
        part = pl.ds(c * step_x, step_x)
        return pltpu.make_async_remote_copy(
            src_ref=cur.at[part] if own else xout.at[m, part],
            dst_ref=xout.at[m, part],
            send_sem=ssem,
            recv_sem=xrecv.at[m, c],
            device_id=(bi, to),
            device_id_type=MESH,
        )

    def phase(p, c, drain):
        def go(copy):
            copy.wait_send() if drain else copy.start()

        def arrived_w(b):
            if not drain:
                wcopy(False, b, c, bi, wup.at[0, c]).wait_recv()

        if p == 0:
            @pl.when(l < nl - 1)
            def _():
                go(wcopy(True, bi, c, group(l + 1, q), wup.at[0, c]))

            @pl.when(l > 0)
            def _():
                go(wcopy(True, bi, c, group(l - 1, q), wdn.at[0, c]))

            for i, side in enumerate(sides):
                go(wcopy(True, bi, c, group(l, side), wcross.at[i, l, c]))
            for i, m in enumerate(fars):
                go(xcopy(True, mi, c, m, xfar.at[i, c]))
            for i, m in enumerate(partners):
                go(xcopy(True, mi, c, m, xcore.at[i, y, c]))
        else:
            @pl.when(l - p >= 0)
            def _():
                b = group(l - p, q)
                arrived_w(b)

                @pl.when(l < nl - 1)
                def _():
                    go(wcopy(False, b, c, group(l + 1, q), wup.at[p, c]))

                def across():
                    for i, side in enumerate(sides):
                        go(wcopy(False, b, c, group(l, side), wcross.at[i, l - p, c]))

                if halves and p == 1:
                    pl.when((l < nl // 2) | (c < first))(across)
                else:
                    across()

            @pl.when(l + p <= nl - 1)
            def _():
                b = group(l + p, q)
                arrived_w(b)

                @pl.when(l > 0)
                def _():
                    go(wcopy(False, b, c, group(l - 1, q), wdn.at[p, c]))

                def across():
                    for i, side in enumerate(sides):
                        go(wcopy(False, b, c, group(l, side), wcross.at[i, l + p, c]))

                if halves and p == 1:
                    pl.when((l >= nl // 2) | (c < first))(across)
                else:
                    across()

            if halves and p == 1:
                @pl.when(c >= first)
                def _():
                    b = group(l, sides[0])
                    arrived_w(b)

                    @pl.when((l + 1 >= nl // 2) & (l < nl - 1))
                    def _():
                        go(wcopy(False, b, c, group(l + 1, q), whalf.at[0, c]))

                    @pl.when((l - 1 < nl // 2) & (l > 0))
                    def _():
                        go(wcopy(False, b, c, group(l - 1, q), whalf.at[1, c]))

        if p == nl - 1:
            for d, far in enumerate(fars):
                if not drain:
                    xcopy(False, far, c, mi, xfar.at[0, c]).wait_recv()
                for i, m in enumerate(partners):
                    go(xcopy(False, far, c, m, xcore.at[i, far // nc, c]))

    for p in range(nl):
        @pl.loop(0, pieces)
        def _(c, p=p):
            phase(p, c, False)

        if p == 0:
            in_w.wait()
            in_x.wait()
            out_w = pltpu.make_async_copy(wv, wout.at[bi], lsem.at[2])
            out_x = pltpu.make_async_copy(xv, xout.at[mi], lsem.at[3])
            out_w.start()
            out_x.start()

    @pl.loop(0, pieces)
    def _(c):
        for side in sides:
            for level in range(nl):
                b = group(level, side)

                def arrive(b=b):
                    wcopy(False, b, c, bi, wup.at[0, c]).wait_recv()

                if halves:
                    pl.when((l != level) | (c < first))(arrive)
                else:
                    arrive()
        for m in partners:
            for yy in range(ny):
                xcopy(False, yy * nc + m % nc, c, mi, xfar.at[0, c]).wait_recv()

    out_w.wait()
    out_x.wait()
    for p in range(nl):
        @pl.loop(0, pieces)
        def _(c, p=p):
            phase(p, c, True)


def gather(geo, shards, groups, layer, tiles, cur):
    nl, nq, _, nc = geo
    pieces = 8 if groups <= 8 else 2
    ny = shards // nc
    dma = pltpu.SemaphoreType.DMA
    return pl.pallas_call(
        functools.partial(gather_kernel, geo, shards, layer, pieces),
        out_shape=(
            jax.ShapeDtypeStruct((groups,) + tiles.shape[1:], tiles.dtype),
            jax.ShapeDtypeStruct((shards,) + cur.shape, cur.dtype),
        ),
        in_specs=[pl.BlockSpec(memory_space=pl.ANY)] * 2,
        out_specs=(pl.BlockSpec(memory_space=pl.ANY),) * 2,
        scratch_shapes=[
            pltpu.VMEM(tiles.shape[1:], tiles.dtype),
            pltpu.VMEM(cur.shape, cur.dtype),
            dma((4,)),
            dma((groups, pieces)),
            dma((nl, pieces)),
            dma((nl, pieces)),
            dma((max(nq - 1, 1), nl, pieces)),
            dma((2, pieces)),
            dma((shards, pieces)),
            dma((max(ny - 1, 1), pieces)),
            dma((max(nc - 1, 1), ny, pieces)),
        ],
        compiler_params=pltpu.CompilerParams(collective_id=layer, has_side_effects=True),
        name=f"gather_{layer}",
    )(tiles, cur)


def layer_kernel(fan, batch_blocks, steps, ids, x_ref, w_ref, b_ref, o_ref, r_ref, s_ref):
    step = pl.program_id(0) * steps + pl.program_id(1)
    side = w_ref.shape[4]

    @pl.when(step == 0)
    def _():
        s_ref[...] = jnp.zeros_like(s_ref)

    for j in range(batch_blocks):
        xs, ws = [], []
        for t in range(fan):
            at = ids[(step * batch_blocks + j) * fan + t]
            xs.append(x_ref[0, :, pl.ds(pl.multiple_of(at * side, side), side)])
            ws.append(w_ref[:, j, t].reshape(side, side))
        total = jnp.dot(
            jnp.concatenate(xs, axis=1),
            jnp.concatenate(ws, axis=0),
            preferred_element_type=jnp.float32,
        )
        cols = slice(j * side, (j + 1) * side)
        out = jnp.clip(total + b_ref[:, cols], 0.0, 32.0).astype(o_ref.dtype)
        o_ref[:, cols] = out
        s_ref[...] += out.astype(jnp.float32)

    @pl.when(step == pl.num_programs(0) * steps - 1)
    def _():
        line = jnp.sum(s_ref[...].T, axis=0, keepdims=True)
        r_ref[...] = jnp.broadcast_to(line, r_ref.shape)


def apply_layer(ids, xall, wall, bias, blocks):
    shards, rows, width = xall.shape
    groups, cb, fan, share, side = wall.shape
    per_shard = cb // shards
    batch_blocks = min(blocks, per_shard)
    steps = per_shard // batch_blocks
    return pl.pallas_call(
        functools.partial(layer_kernel, fan, batch_blocks, steps),
        out_shape=(
            jax.ShapeDtypeStruct((rows, width), xall.dtype),
            jax.ShapeDtypeStruct((8, rows), jnp.float32),
        ),
        grid_spec=pltpu.PrefetchScalarGridSpec(
            num_scalar_prefetch=1,
            grid=(shards, steps),
            in_specs=[
                pl.BlockSpec((1, rows, width), lambda s, k, ids: (s, 0, 0)),
                pl.BlockSpec(
                    (groups, batch_blocks, fan, share, side),
                    lambda s, k, ids: (0, s * steps + k, 0, 0, 0),
                ),
                pl.BlockSpec((1, batch_blocks * side), lambda s, k, ids: (0, s * steps + k)),
            ],
            out_specs=(
                pl.BlockSpec((rows, batch_blocks * side), lambda s, k, ids: (0, s * steps + k)),
                pl.BlockSpec((8, rows), lambda s, k, ids: (0, 0)),
            ),
            scratch_shapes=[pltpu.VMEM((rows, side), jnp.float32)],
        ),
        compiler_params=pltpu.CompilerParams(
            dimension_semantics=("arbitrary", "arbitrary"), vmem_limit_bytes=48 * 1024 * 1024
        ),
    )(ids, xall, wall, bias)


def means_kernel(groups, shards, neurons, x_ref, rows_ref, all_ref, slots, ssem, rsem):
    bi = lax.axis_index("batch")
    mi = lax.axis_index("mp")
    me = bi * shards + mi
    total = groups * shards
    barrier = pltpu.get_barrier_semaphore()

    def peer(d):
        to = (me + d) % total
        return to // shards, to % shards

    @pl.loop(1, total)
    def _(d):
        pl.semaphore_signal(barrier, inc=1, device_id=peer(d), device_id_type=MESH)

    pl.semaphore_wait(barrier, total - 1)

    def copy(d, slot):
        return pltpu.make_async_remote_copy(
            src_ref=x_ref,
            dst_ref=slots.at[slot],
            send_sem=ssem.at[d],
            recv_sem=rsem.at[slot],
            device_id=peer(d),
            device_id_type=MESH,
        )

    @pl.loop(1, total)
    def _(d):
        copy(d, me).start()

    slots[me] = x_ref[...]

    @pl.loop(1, total)
    def _(d):
        copy(d, (me + d) % total).wait_recv()

    whole = jnp.zeros(all_ref.shape, jnp.float32)
    for b in range(groups):
        one = slots[b * shards]
        for m in range(1, shards):
            one = one + slots[b * shards + m]
        whole = whole + one / neurons
    all_ref[...] = whole
    mine = slots[bi * shards]
    for m in range(1, shards):
        mine = mine + slots[bi * shards + m]
    rows_ref[...] = mine / neurons

    @pl.loop(1, total)
    def _(d):
        copy(d, me).wait_send()


def means(groups, shards, neurons, sums):
    total = groups * shards
    if total > 64:
        shard_sum = lax.psum(sums[0], "mp") / neurons
        return shard_sum, lax.psum(shard_sum, "batch")
    vmem = pl.BlockSpec(memory_space=pltpu.VMEM)
    like = jax.ShapeDtypeStruct(sums.shape, jnp.float32)
    mine, whole = pl.pallas_call(
        functools.partial(means_kernel, groups, shards, neurons),
        out_shape=(like, like),
        in_specs=[vmem],
        out_specs=(vmem, vmem),
        scratch_shapes=[
            pltpu.VMEM((total,) + sums.shape, jnp.float32),
            pltpu.SemaphoreType.DMA((total,)),
            pltpu.SemaphoreType.DMA((total,)),
        ],
        compiler_params=pltpu.CompilerParams(collective_id=20, has_side_effects=True),
        name="means",
    )(sums)
    return mine[0], whole[0]


def on_device(geo, features, tiles, biases, in_block):
    shards = lax.axis_size("mp")
    groups = lax.axis_size("batch")
    me = lax.axis_index("mp")
    rows = features.shape[0]
    side = tiles.shape[4]
    cb = tiles.shape[1]
    fan = tiles.shape[2]
    current = features
    mine = lax.dynamic_slice_in_dim(in_block, me * cb, cb, axis=1) % cb
    for layer in range(tiles.shape[0]):
        wall, xall = gather(geo, shards, groups, layer, tiles, current)
        current, sums = apply_layer(
            mine[layer].reshape(-1), xall, wall, biases[layer].reshape(1, -1), 8
        )
    row_means, whole = means(groups, shards, cb * side * shards, sums)
    grand = jnp.sum(whole) / (rows * groups)
    return (current, row_means, grand)


def solution(mesh):
    placed = (P("batch", "mp"), P(None, "mp", None, "batch", None), P(None, "mp"), P())
    return jax.shard_map(
        functools.partial(on_device, geometry(mesh)),
        mesh=mesh,
        in_specs=placed,
        out_specs=(P("batch", "mp"), P("batch"), P()),
        check_vma=False,
    )
```

```python
import functools
import math

import jax
import jax.numpy as jnp
from jax import lax
from jax.experimental import pallas as pl
from jax.experimental.pallas import tpu as pltpu
from jax.sharding import PartitionSpec as P

MESH = pl.DeviceIdType.MESH


def geometry(mesh):
    groups, shards = mesh.devices.shape
    where = [getattr(d, "coords", None) for d in mesh.devices[:, 0]]
    if groups == 1 or where[0] is None or where[0] == where[1]:
        return groups, 1, True, 1
    moved = [i for i in range(len(where[0])) if where[0][i] != where[1][i]][0]
    minor = 1
    while minor < groups and all(
        where[minor][i] == where[0][i] for i in range(len(where[0])) if i != moved
    ):
        minor += 1
    major = groups // minor
    row = [d.coords for d in mesh.devices[0, :]]
    cores = sum(1 for c in row if c == row[0])
    if major >= minor:
        return major, minor, True, cores
    return minor, major, False, cores


def gather_kernel(
    geo, shards, layer, pieces,
    tiles, cur, wout, xout,
    wv, xv, lsem, wrecv, wup, wdn, wcross, whalf, xrecv, xfar, xcore,
):
    nl, nq, line_major, nc = geo
    ny = shards // nc
    bi = lax.axis_index("batch")
    mi = lax.axis_index("mp")
    if line_major:
        l, q = bi // nq, bi % nq
    else:
        l, q = bi % nl, bi // nl
    y, core = mi // nc, mi % nc
    step_w = tiles.shape[1] // pieces
    step_x = cur.shape[0] // pieces
    halves = nq == 2 and nl % 2 == 0
    first = pieces // 2

    def group(level, side):
        return level * nq + side if line_major else side * nl + level

    sides = [(q + d) % nq for d in range(1, nq)]
    fars = [((y + d) % ny) * nc + core for d in range(1, ny)]
    partners = [y * nc + (core + d) % nc for d in range(1, nc)]

    barrier = pltpu.get_barrier_semaphore()

    def greet(b, m):
        pl.semaphore_signal(barrier, inc=1, device_id=(b, m), device_id_type=MESH)

    @pl.when(l > 0)
    def _():
        greet(group(l - 1, q), mi)

    @pl.when(l < nl - 1)
    def _():
        greet(group(l + 1, q), mi)

    for side in sides:
        greet(group(l, side), mi)
    for m in fars + partners:
        greet(bi, m)
    near = jnp.where(l > 0, 1, 0) + jnp.where(l < nl - 1, 1, 0)
    pl.semaphore_wait(barrier, len(sides) + len(fars) + len(partners) + near)

    in_w = pltpu.make_async_copy(tiles.at[layer], wv, lsem.at[0])
    in_x = pltpu.make_async_copy(cur, xv, lsem.at[1])
    in_w.start()
    in_x.start()

    def wcopy(own, b, c, to, ssem):
        part = pl.ds(c * step_w, step_w)
        return pltpu.make_async_remote_copy(
            src_ref=tiles.at[layer, part] if own else wout.at[b, part],
            dst_ref=wout.at[b, part],
            send_sem=ssem,
            recv_sem=wrecv.at[b, c],
            device_id=(to, mi),
            device_id_type=MESH,
        )

    def xcopy(own, m, c, to, ssem):
        part = pl.ds(c * step_x, step_x)
        return pltpu.make_async_remote_copy(
            src_ref=cur.at[part] if own else xout.at[m, part],
            dst_ref=xout.at[m, part],
            send_sem=ssem,
            recv_sem=xrecv.at[m, c],
            device_id=(bi, to),
            device_id_type=MESH,
        )

    def phase(p, c, drain):
        def go(copy):
            copy.wait_send() if drain else copy.start()

        def arrived_w(b):
            if not drain:
                wcopy(False, b, c, bi, wup.at[0, c]).wait_recv()

        if p == 0:
            @pl.when(l < nl - 1)
            def _():
                go(wcopy(True, bi, c, group(l + 1, q), wup.at[0, c]))

            @pl.when(l > 0)
            def _():
                go(wcopy(True, bi, c, group(l - 1, q), wdn.at[0, c]))

            for i, side in enumerate(sides):
                go(wcopy(True, bi, c, group(l, side), wcross.at[i, l, c]))
            for i, m in enumerate(fars):
                go(xcopy(True, mi, c, m, xfar.at[i, c]))
            for i, m in enumerate(partners):
                go(xcopy(True, mi, c, m, xcore.at[i, y, c]))
        else:
            @pl.when(l - p >= 0)
            def _():
                b = group(l - p, q)
                arrived_w(b)

                @pl.when(l < nl - 1)
                def _():
                    go(wcopy(False, b, c, group(l + 1, q), wup.at[p, c]))

                def across():
                    for i, side in enumerate(sides):
                        go(wcopy(False, b, c, group(l, side), wcross.at[i, l - p, c]))

                if halves and p == 1:
                    pl.when((l < nl // 2) | (c < first))(across)
                else:
                    across()

            @pl.when(l + p <= nl - 1)
            def _():
                b = group(l + p, q)
                arrived_w(b)

                @pl.when(l > 0)
                def _():
                    go(wcopy(False, b, c, group(l - 1, q), wdn.at[p, c]))

                def across():
                    for i, side in enumerate(sides):
                        go(wcopy(False, b, c, group(l, side), wcross.at[i, l + p, c]))

                if halves and p == 1:
                    pl.when((l >= nl // 2) | (c < first))(across)
                else:
                    across()

            if halves and p == 1:
                @pl.when(c >= first)
                def _():
                    b = group(l, sides[0])
                    arrived_w(b)

                    @pl.when((l + 1 >= nl // 2) & (l < nl - 1))
                    def _():
                        go(wcopy(False, b, c, group(l + 1, q), whalf.at[0, c]))

                    @pl.when((l - 1 < nl // 2) & (l > 0))
                    def _():
                        go(wcopy(False, b, c, group(l - 1, q), whalf.at[1, c]))

        if p == nl - 1:
            for d, far in enumerate(fars):
                if not drain:
                    xcopy(False, far, c, mi, xfar.at[0, c]).wait_recv()
                for i, m in enumerate(partners):
                    go(xcopy(False, far, c, m, xcore.at[i, far // nc, c]))

    for p in range(nl):
        @pl.loop(0, pieces)
        def _(c, p=p):
            phase(p, c, False)

        if p == 0:
            in_w.wait()
            in_x.wait()
            out_w = pltpu.make_async_copy(wv, wout.at[bi], lsem.at[2])
            out_x = pltpu.make_async_copy(xv, xout.at[mi], lsem.at[3])
            out_w.start()
            out_x.start()

    @pl.loop(0, pieces)
    def _(c):
        for side in sides:
            for level in range(nl):
                b = group(level, side)

                def arrive(b=b):
                    wcopy(False, b, c, bi, wup.at[0, c]).wait_recv()

                if halves:
                    pl.when((l != level) | (c < first))(arrive)
                else:
                    arrive()
        for m in partners:
            for yy in range(ny):
                xcopy(False, yy * nc + m % nc, c, mi, xfar.at[0, c]).wait_recv()

    out_w.wait()
    out_x.wait()
    for p in range(nl):
        @pl.loop(0, pieces)
        def _(c, p=p):
            phase(p, c, True)


def gather(geo, shards, groups, layer, tiles, cur):
    nl, nq, _, nc = geo
    pieces = 8 if groups <= 8 else 2
    ny = shards // nc
    dma = pltpu.SemaphoreType.DMA
    return pl.pallas_call(
        functools.partial(gather_kernel, geo, shards, layer, pieces),
        out_shape=(
            jax.ShapeDtypeStruct((groups,) + tiles.shape[1:], tiles.dtype),
            jax.ShapeDtypeStruct((shards,) + cur.shape, cur.dtype),
        ),
        in_specs=[pl.BlockSpec(memory_space=pl.ANY)] * 2,
        out_specs=(pl.BlockSpec(memory_space=pl.ANY),) * 2,
        scratch_shapes=[
            pltpu.VMEM(tiles.shape[1:], tiles.dtype),
            pltpu.VMEM(cur.shape, cur.dtype),
            dma((4,)),
            dma((groups, pieces)),
            dma((nl, pieces)),
            dma((nl, pieces)),
            dma((max(nq - 1, 1), nl, pieces)),
            dma((2, pieces)),
            dma((shards, pieces)),
            dma((max(ny - 1, 1), pieces)),
            dma((max(nc - 1, 1), ny, pieces)),
        ],
        compiler_params=pltpu.CompilerParams(collective_id=layer, has_side_effects=True),
        name=f"gather_{layer}",
    )(tiles, cur)


def layer_kernel(ids, x_ref, w_ref, b_ref, o_ref, r_ref, xl, wl, s_ref, loads):
    shards, rows, _ = x_ref.shape
    _, cb, fan, _, side = w_ref.shape
    per_shard = cb // shards
    width = math.gcd(per_shard, 8)

    def pulls(s):
        part = pl.ds(s * per_shard, per_shard)
        return (
            pltpu.make_async_copy(x_ref.at[s], xl.at[s], loads.at[0, s]),
            pltpu.make_async_copy(w_ref.at[:, part], wl.at[:, part], loads.at[1, s]),
        )

    for s in range(min(2, shards)):
        for pull in pulls(s):
            pull.start()
    s_ref[...] = jnp.zeros_like(s_ref)
    for s in range(shards):
        for pull in pulls(s):
            pull.wait()
        if s + 2 < shards:
            for pull in pulls(s + 2):
                pull.start()

        @pl.loop(0, per_shard // width)
        def _(k, s=s):
            for jj in range(width):
                j = s * per_shard + k * width + jj
                xs, ws = [], []
                for t in range(fan):
                    at = ids[j * fan + t]
                    xs.append(xl[s, :, pl.ds(pl.multiple_of(at * side, side), side)])
                    ws.append(wl[:, j, t].reshape(side, side))
                total = jnp.dot(
                    jnp.concatenate(xs, axis=1),
                    jnp.concatenate(ws, axis=0),
                    preferred_element_type=jnp.float32,
                )
                cols = pl.ds(pl.multiple_of(j * side, side), side)
                out = jnp.clip(total + b_ref[:, cols], 0.0, 32.0).astype(o_ref.dtype)
                o_ref[:, cols] = out
                s_ref[...] += out.astype(jnp.float32)

    line = jnp.sum(s_ref[...].T, axis=0, keepdims=True)
    r_ref[...] = jnp.broadcast_to(line, r_ref.shape)


def apply_layer(ids, xall, wall, bias):
    shards, rows, width = xall.shape
    side = wall.shape[4]
    hbm = pl.BlockSpec(memory_space=pl.ANY)
    vmem = pl.BlockSpec(memory_space=pltpu.VMEM)
    return pl.pallas_call(
        layer_kernel,
        out_shape=(
            jax.ShapeDtypeStruct((rows, width), xall.dtype),
            jax.ShapeDtypeStruct((8, rows), jnp.float32),
        ),
        in_specs=[pl.BlockSpec(memory_space=pltpu.SMEM), hbm, hbm, vmem],
        out_specs=(vmem, vmem),
        scratch_shapes=[
            pltpu.VMEM(xall.shape, xall.dtype),
            pltpu.VMEM(wall.shape, wall.dtype),
            pltpu.VMEM((rows, side), jnp.float32),
            pltpu.SemaphoreType.DMA((2, shards)),
        ],
        compiler_params=pltpu.CompilerParams(vmem_limit_bytes=52 * 1024 * 1024),
        name="layer",
    )(ids, xall, wall, bias)


def means_kernel(groups, shards, neurons, x_ref, rows_ref, all_ref, slots, ssem, rsem):
    bi = lax.axis_index("batch")
    mi = lax.axis_index("mp")
    me = bi * shards + mi
    total = groups * shards
    barrier = pltpu.get_barrier_semaphore()

    def peer(d):
        to = (me + d) % total
        return to // shards, to % shards

    @pl.loop(1, total)
    def _(d):
        pl.semaphore_signal(barrier, inc=1, device_id=peer(d), device_id_type=MESH)

    pl.semaphore_wait(barrier, total - 1)

    def copy(d, slot):
        return pltpu.make_async_remote_copy(
            src_ref=x_ref,
            dst_ref=slots.at[slot],
            send_sem=ssem.at[d],
            recv_sem=rsem.at[slot],
            device_id=peer(d),
            device_id_type=MESH,
        )

    @pl.loop(1, total)
    def _(d):
        copy(d, me).start()

    slots[me] = x_ref[...]

    @pl.loop(1, total)
    def _(d):
        copy(d, (me + d) % total).wait_recv()

    whole = jnp.zeros(all_ref.shape, jnp.float32)
    for b in range(groups):
        one = slots[b * shards]
        for m in range(1, shards):
            one = one + slots[b * shards + m]
        whole = whole + one / neurons
    all_ref[...] = whole
    mine = slots[bi * shards]
    for m in range(1, shards):
        mine = mine + slots[bi * shards + m]
    rows_ref[...] = mine / neurons

    @pl.loop(1, total)
    def _(d):
        copy(d, me).wait_send()


def means(groups, shards, neurons, sums):
    total = groups * shards
    if total > 64:
        shard_sum = lax.psum(sums[0], "mp") / neurons
        return shard_sum, lax.psum(shard_sum, "batch")
    vmem = pl.BlockSpec(memory_space=pltpu.VMEM)
    like = jax.ShapeDtypeStruct(sums.shape, jnp.float32)
    mine, whole = pl.pallas_call(
        functools.partial(means_kernel, groups, shards, neurons),
        out_shape=(like, like),
        in_specs=[vmem],
        out_specs=(vmem, vmem),
        scratch_shapes=[
            pltpu.VMEM((total,) + sums.shape, jnp.float32),
            pltpu.SemaphoreType.DMA((total,)),
            pltpu.SemaphoreType.DMA((total,)),
        ],
        compiler_params=pltpu.CompilerParams(collective_id=20, has_side_effects=True),
        name="means",
    )(sums)
    return mine[0], whole[0]


def on_device(geo, features, tiles, biases, in_block):
    shards = lax.axis_size("mp")
    groups = lax.axis_size("batch")
    me = lax.axis_index("mp")
    rows = features.shape[0]
    side = tiles.shape[4]
    cb = tiles.shape[1]
    fan = tiles.shape[2]
    current = features
    mine = lax.dynamic_slice_in_dim(in_block, me * cb, cb, axis=1) % cb
    for layer in range(tiles.shape[0]):
        wall, xall = gather(geo, shards, groups, layer, tiles, current)
        current, sums = apply_layer(
            mine[layer].reshape(-1), xall, wall, biases[layer].reshape(1, -1)
        )
    row_means, whole = means(groups, shards, cb * side * shards, sums)
    grand = jnp.sum(whole) / (rows * groups)
    return (current, row_means, grand)


def solution(mesh):
    placed = (P("batch", "mp"), P(None, "mp", None, "batch", None), P(None, "mp"), P())
    return jax.shard_map(
        functools.partial(on_device, geometry(mesh)),
        mesh=mesh,
        in_specs=placed,
        out_specs=(P("batch", "mp"), P("batch"), P()),
        check_vma=False,
    )
```
